32 devices in a mesh: groups: 1, rail: 16 (over z, y, x), node: 2 (over core).
Axes of the slice: x: 2, y: 2, z: 4, core: 2. Of those that a mesh axis runs over, the one named last changes fastest.
Arguments:
- tokens: bfloat16 [512, 7168], P(('groups', 'rail', 'node')), may hold values from -6 to 6
- routes: int32 [512, 2], P(('groups', 'rail', 'node')), may hold values from 0 to 3, all different within a row; in each aligned block of 16 rows (0 to 15, 16 to 31, ...) at most 12 rows name the same one
- route_weight: int32 [512, 2], P(('groups', 'rail', 'node')), may hold values from 1 to 255
- gate_weight: bfloat16 [16, 2, 7168, 256], P('rail', 'node'), may hold values from -0.0625 to 0.0625
- up_weight: bfloat16 [16, 2, 7168, 256], P('rail', 'node'), may hold values from -0.0625 to 0.0625
- down_weight: bfloat16 [16, 2, 256, 7168], P('rail', 'node'), may hold values from -0.125 to 0.125
Outputs:
- moe_out: bfloat16 [512, 7168], P(('groups', 'rail', 'node'))
The draws below stay inside these ranges and needn't reach their ends.
Inputs may be any that keep to these rules, and one draw needn't show every extreme that they name: `routes`: each row names 2 different experts; among the 16 rows of one device no expert is named by more than 12 rows, and in some blocks of every draw an expert is named by exactly 12.
All inputs are finite; a program needn't handle non-finite values.
Results may differ from the reference program's by a relative error of at most 0.0085.
Values may be sent and summed in bfloat16 or wider, within the bound.
No kernel may reach another device: no remote copies, remote signals or barrier semaphores. Data moves between devices by JAX's collectives and lax.ppermute only.
A program may use at most 128 MiB of HBM per device.

```python
import math
import jax
import jax.numpy as jnp
import numpy as np
from jax import lax

D = 7168
HID = 2048
SLICES = 8
TOP = 2
TOK_DEV = 16
EXPERTS = 4
CAP = 12
TOKENS = 512
N_RAIL = 16
N_NODE = 2


def place_ends(entries, rng, smallest, high):
    longest = entries.shape.index(max(entries.shape))
    spots = []
    for shift in (0, 1):
        where = [jax.random.randint(jax.random.fold_in(rng, axis), (), 0, length) for axis, length in enumerate(entries.shape)]
        where[longest] = (where[longest] + shift) % entries.shape[longest]
        spots.append(tuple(where))
    return entries.at[spots[0]].set(smallest).at[spots[1]].set(high)


def block_levels(rng, extent, split, low, largest):
    level, own = 1.0, jax.random.fold_in(rng, 6)
    for axis_at, blocks in split:
        steps = jnp.exp(jax.random.uniform(jax.random.fold_in(own, axis_at), (blocks,), jnp.float32, low / len(split), largest / len(split)))
        level = level * jnp.repeat(steps, extent[axis_at] // blocks).reshape([-1 if axis == axis_at else 1 for axis in range(len(extent))])
    return level


def routed_block(key, own, number, rows, number_of, top, bound, lean):
    ranking = jax.random.permutation(key, number_of)
    packed, common = load_shares(number_of, rows * top, bound, lean, True), load_shares(number_of, rows * top, bound, lean, False)
    places = jnp.arange(number_of)

    def named(lengths, rotation):
        used = int((lengths > 0).sum())
        fixed = max(1, used // 4)
        passed = fixed + (places - fixed + rotation * (used - fixed)) % max(1, number_of - fixed)
        return jnp.zeros((number_of,), jnp.int32).at[ranking[jnp.where(places < fixed, places, passed)]].set(jnp.asarray(lengths, jnp.int32))

    lengths = jnp.where(number % 4 == 0, named(packed, number // 4), named(common, number - number // 4 - 1))
    mixed = jax.random.permutation(jax.random.fold_in(own, 3), number_of)
    giver, sink = mixed[0:number_of // 2 * 2:2], mixed[1:number_of // 2 * 2:2]
    margin = jnp.minimum(lengths[giver] - 1, bound - lengths[sink]) // 2
    margin = jnp.where((giver == ranking[0]) | (sink == ranking[0]) | (lengths[sink] == 0), 0, jnp.maximum(margin, 0))
    passed = jax.random.randint(jax.random.fold_in(own, 4), (number_of // 2,), 0, 1 << 20) % (margin + 1)
    lengths = lengths.at[giver].add(-passed).at[sink].add(passed)
    members = jnp.searchsorted(jnp.cumsum(lengths), jnp.arange(rows * top), side="right").astype(jnp.int32)
    grid = members.reshape(top, rows).T
    grid = grid[jax.random.permutation(jax.random.fold_in(own, 1), rows)]
    rotation = jax.random.randint(jax.random.fold_in(own, 2), (rows, 1), 0, top)
    return jnp.take_along_axis(grid, (jnp.arange(top)[None, :] + rotation) % top, axis=1)


def load_shares(number_of, total, bound, lean, full):
    portions = [(1 << 20) // math.isqrt(rank ** lean) + 1 for rank in range(1, number_of + 1)]
    largest = bound if full else min(bound, max(-(-total // number_of), total * portions[0] // sum(portions)))
    least = 1 if total - largest >= number_of - 1 else 0
    holding, rest = [largest] + [least] * (number_of - 1), total - largest - least * (number_of - 1)
    while rest > 0:
        movable = [i for i in range(1, number_of) if holding[i] < largest] or [i for i in range(1, number_of) if holding[i] < bound]
        whole, remaining = sum([portions[i] for i in movable]), rest
        for i in movable:
            extra = min(bound - holding[i], max(1, remaining * portions[i] // whole), rest)
            holding[i] = holding[i] + extra
            rest = rest - extra
    return np.array(holding)


def gaussian(own_key, dims, deviation, limit, shards=(), held_as=jnp.bfloat16):
    entries = jax.random.normal(own_key, dims, jnp.float32) * deviation
    if len(shards) > 0:
        entries = block_levels(own_key, dims, shards, -0.22, 0.18) * entries
    return jnp.clip(entries, min=-limit, max=limit).astype(held_as)


def setup_inputs(seed: int = 0, part: int = 0) -> dict:
    streams_of = jax.random.split(jax.random.key(seed), 7)
    part_splits = jax.random.split(jax.random.fold_in(streams_of[6], part), 7)
    tokens = gaussian(part_splits[0], (TOKENS, D), 1.0, 6.0, ((0, 32),))
    routes_keys = jax.random.split(jax.random.fold_in(part_splits[1], 1), TOKENS // TOK_DEV)
    routes_turns = jax.random.permutation(jax.random.fold_in(part_splits[1], 3), TOKENS // TOK_DEV)
    routes = jax.vmap(lambda own, number: routed_block(jax.random.fold_in(part_splits[1], 2), own, number, TOK_DEV, EXPERTS, TOP, CAP, 2))(routes_keys, routes_turns).reshape((TOKENS, TOP))
    route_weight = place_ends(jax.random.randint(part_splits[2], (TOKENS, TOP), 1, 256), jax.random.fold_in(part_splits[2], 1), 1, 255).astype(jnp.int32)
    gate_weight = gaussian(streams_of[3], (N_RAIL, N_NODE, D, HID // SLICES), D ** -0.5, 0.0625, ((0, 16), (1, 2)))
    up_weight = gaussian(streams_of[4], (N_RAIL, N_NODE, D, HID // SLICES), D ** -0.5, 0.0625, ((0, 16), (1, 2)))
    down_weight = gaussian(streams_of[5], (N_RAIL, N_NODE, HID // SLICES, D), HID ** -0.5, 0.125, ((0, 16), (1, 2)))
    return {"tokens": tokens, "routes": routes, "route_weight": route_weight, "gate_weight": gate_weight, "up_weight": up_weight, "down_weight": down_weight}


def slot_numbers(routes):
    blocks = routes.reshape(-1, TOK_DEV * TOP)
    onehot = (blocks[:, :, None] == jnp.arange(EXPERTS, dtype=jnp.int32)[None, None, :]).astype(jnp.int32)
    earlier = jnp.cumsum(onehot, axis=1) - onehot
    return jnp.sum(earlier * onehot, axis=2).astype(jnp.int32)


def arrange(weight):
    split_count = N_RAIL // SLICES
    shaped = weight.reshape(split_count, SLICES, N_NODE, weight.shape[2], weight.shape[3])
    return shaped.transpose(0, 2, 1, 3, 4).reshape(EXPERTS, SLICES, weight.shape[2], weight.shape[3])


def reference(tokens, routes, route_weight, gate_weight, up_weight, down_weight):
    block_count = TOKENS // TOK_DEV
    slot_of = slot_numbers(routes)
    local_row = jnp.broadcast_to((jnp.arange(TOK_DEV * TOP, dtype=jnp.int32) // TOP)[None, :], slot_of.shape)
    block_ids = jnp.broadcast_to(jnp.arange(block_count, dtype=jnp.int32)[:, None], slot_of.shape)
    token_of = jnp.zeros((EXPERTS, block_count, CAP), jnp.int32)
    token_of = token_of.at[routes.reshape(block_count, -1), block_ids, slot_of].set(local_row + 1)

    def expert_rows(items):
        owner, w_gate, w_up, w_down = items
        global_row = jnp.arange(block_count, dtype=jnp.int32)[:, None] * TOK_DEV + owner - 1
        picked = tokens[jnp.maximum(global_row, 0)]
        inputs = jnp.where((owner > 0)[:, :, None], picked, jnp.zeros((), tokens.dtype)).reshape(-1, D)
        wide = inputs.astype(jnp.float32)
        gate_vals = jnp.einsum("rd,sdh->srh", wide, w_gate.astype(jnp.float32))
        up_vals = jnp.einsum("rd,sdh->srh", wide, w_up.astype(jnp.float32))
        hidden = (jax.nn.silu(gate_vals) * up_vals).astype(jnp.bfloat16)
        partial_value = jnp.einsum("srh,shd->srd", hidden.astype(jnp.float32), w_down.astype(jnp.float32))
        summed = jnp.sum(partial_value, axis=0)
        return summed.reshape(block_count, CAP, D)

    results = lax.map(expert_rows, (token_of, arrange(gate_weight), arrange(up_weight), arrange(down_weight)))
    block_of = (jnp.arange(TOKENS, dtype=jnp.int32) // TOK_DEV)[:, None]
    chosen = results[routes, block_of, slot_of.reshape(TOKENS, TOP)]
    share = route_weight.astype(jnp.float32) / 256.0
    return jnp.sum(share[:, :, None] * chosen, axis=1).astype(jnp.bfloat16)
```

```python
import jax
import jax.numpy as jnp
from jax import lax
from jax.sharding import PartitionSpec as P

SLICES = 8
LANES = 128
PLANE = 4


def send(block, target):
    rails, nodes = lax.axis_size("rail"), lax.axis_size("node")
    route = []
    for rail in range(rails):
        for node in range(nodes):
            rail_to, node_to = target(rail, node)
            route.append((rail * nodes + node, rail_to * nodes + node_to))
    return lax.ppermute(block, ("rail", "node"), route)


def first_partner(rail, node):
    return rail ^ (1 if node % 2 == 0 else 2), node


def second_partner(rail, node):
    return rail ^ (2 if node % 2 == 0 else 1), node


def layer_shift(layers, count):
    def target(rail, node):
        return (rail // PLANE + count) % layers * PLANE + rail % PLANE, node

    return target


def node_shift(nodes, count):
    return lambda rail, node: (rail, (node + count) % nodes)


def shards(tokens, routes, route_weight, gate_weight, up_weight, down_weight):
    row_count, model_width = tokens.shape
    nodes = lax.axis_size("node")
    layers = lax.axis_size("rail") // PLANE
    node = lax.axis_index("node")
    first_expert = lax.axis_index("rail") // SLICES * nodes

    weights = []
    for count in range(nodes):
        held = (gate_weight[0, 0], up_weight[0, 0], down_weight[0, 0])
        if count:
            held = tuple(send(w, node_shift(nodes, count)) for w in held)
        weights.append((first_expert + (node - count) % nodes, held))

    lanes = jnp.arange(LANES, dtype=jnp.int32)
    share = route_weight.astype(jnp.float32) / 256.0
    named = routes[:, :, None] == lanes[None, None, :]
    coef = jnp.sum(jnp.where(named, share[:, :, None], 0.0), axis=1).astype(jnp.bfloat16)
    own = jnp.concatenate([tokens, coef], axis=1)

    def experts_of(block):
        rows = block[:, :model_width]
        coefs = block[:, model_width:].astype(jnp.float32)
        total = None
        for expert, (w_gate, w_up, w_down) in weights:
            mine = jnp.sum(jnp.where(lanes[None, :] == expert, coefs, 0.0), axis=1, keepdims=True)
            gate_vals = jnp.dot(rows, w_gate, preferred_element_type=jnp.float32)
            up_vals = jnp.dot(rows, w_up, preferred_element_type=jnp.float32)
            hidden = (jax.nn.silu(gate_vals) * up_vals * mine).astype(jnp.bfloat16)
            part = jnp.dot(hidden, w_down, preferred_element_type=jnp.float32)
            total = part if total is None else total + part
        return total

    shifts = sorted(range(layers), key=lambda count: min(count, layers - count))
    units = [(count, send(own, layer_shift(layers, count)) if count else own) for count in shifts]
    result = None
    for count, unit in units:
        pair = jnp.concatenate([unit, send(unit, first_partner)], axis=0)
        block = jnp.concatenate([pair, send(pair, second_partner)], axis=0)
        out = experts_of(block)
        out = out[: 2 * row_count] + send(out[2 * row_count :].astype(jnp.bfloat16), second_partner)
        out = out[:row_count] + send(out[row_count:].astype(jnp.bfloat16), first_partner)
        if count:
            out = send(out.astype(jnp.bfloat16), layer_shift(layers, -count)).astype(jnp.float32)
        result = out if result is None else result + out
    return result.astype(jnp.bfloat16)


def solution(mesh):
    rows = P(("groups", "rail", "node"), None)
    weights = P("rail", "node", None, None)
    return jax.shard_map(
        shards,
        mesh=mesh,
        in_specs=(rows, rows, rows, weights, weights, weights),
        out_specs=rows,
        check_vma=False,
    )
```

```python
import jax
import jax.numpy as jnp
from jax import lax
from jax.experimental import pallas as pl
from jax.experimental.pallas import tpu as pltpu
from jax.sharding import PartitionSpec as P


SLICES = 8
LANES = 128
PLANE = 4
CHUNK = 1024


def send(block, target):
    rails, nodes = lax.axis_size("rail"), lax.axis_size("node")
    route = []
    for rail in range(rails):
        for node in range(nodes):
            rail_to, node_to = target(rail, node)
            route.append((rail * nodes + node, rail_to * nodes + node_to))
    return lax.ppermute(block, ("rail", "node"), route)


def first_partner(rail, node):
    return rail ^ (1 if node % 2 == 0 else 2), node


def second_partner(rail, node):
    return rail ^ (2 if node % 2 == 0 else 1), node


def layer_shift(layers, count):
    def target(rail, node):
        return (rail // PLANE + count) % layers * PLANE + rail % PLANE, node

    return target


def node_shift(nodes, count):
    return lambda rail, node: (rail, (node + count) % nodes)


def pieces(width):
    return [(start, min(CHUNK, width - start)) for start in range(0, width, CHUNK)]


def experts_kernel(ids, near, far, *refs):
    kept, sent = refs[-2:]
    weights = refs[:-2]
    width = weights[0].shape[0]
    lane = lax.broadcasted_iota(jnp.int32, (1, LANES), 1)
    coefs = jnp.concatenate([near[:, width:], far[:, width:]], axis=0).astype(jnp.float32)
    hidden = []
    for at in range(len(weights) // 3):
        w_gate, w_up, _ = weights[3 * at : 3 * at + 3]
        gate_vals = up_vals = None
        for start, size in pieces(width):
            rows = jnp.concatenate([near[:, start : start + size], far[:, start : start + size]], axis=0)
            gate_part = jnp.dot(rows, w_gate[start : start + size, :], preferred_element_type=jnp.float32)
            up_part = jnp.dot(rows, w_up[start : start + size, :], preferred_element_type=jnp.float32)
            gate_vals = gate_part if gate_vals is None else gate_vals + gate_part
            up_vals = up_part if up_vals is None else up_vals + up_part
        mine = jnp.sum(jnp.where(lane == ids[at], coefs, 0.0), axis=1, keepdims=True)
        silu = gate_vals / (1.0 + jnp.exp(-gate_vals))
        hidden.append((silu * up_vals * mine).astype(jnp.bfloat16))
    count = kept.shape[0]
    for start, size in pieces(width):
        total = None
        for at, value in enumerate(hidden):
            w_down = weights[3 * at + 2]
            part = jnp.dot(value, w_down[:, start : start + size], preferred_element_type=jnp.float32)
            total = part if total is None else total + part
        kept[:, start : start + size] = total[:count]
        sent[:, start : start + size] = total[count:].astype(jnp.bfloat16)


def run_experts(ids, near, far, weights):
    width = weights[0].shape[0]
    rows = near.shape[0]
    flops = 2 * 2 * rows * sum(w.size for w in weights)
    whole = pl.BlockSpec(memory_space=pltpu.VMEM)
    return pl.pallas_call(
        experts_kernel,
        in_specs=[pl.BlockSpec(memory_space=pltpu.SMEM)] + [whole] * (2 + len(weights)),
        out_specs=(whole, whole),
        out_shape=(
            jax.ShapeDtypeStruct((rows, width), jnp.float32),
            jax.ShapeDtypeStruct((rows, width), jnp.bfloat16),
        ),
        cost_estimate=pl.CostEstimate(flops=flops, bytes_accessed=0, transcendentals=0),
        compiler_params=pltpu.CompilerParams(vmem_limit_bytes=40 << 20),
    )(ids, near, far, *weights)


def grouping(layers):
    shifts = sorted(range(1, layers), key=lambda count: min(count, layers - count))
    return [[0]] + [shifts[at : at + 2] for at in range(0, len(shifts), 2)]


def layer(tokens, routes, route_weight, gate_weight, up_weight, down_weight):
    row_count, _ = tokens.shape
    nodes = lax.axis_size("node")
    layers = lax.axis_size("rail") // PLANE
    node = lax.axis_index("node")
    first_expert = lax.axis_index("rail") // SLICES * nodes

    lanes = jnp.arange(LANES, dtype=jnp.int32)
    share = route_weight.astype(jnp.float32) / 256.0
    named = routes[:, :, None] == lanes[None, None, :]
    coef = jnp.sum(jnp.where(named, share[:, :, None], 0.0), axis=1).astype(jnp.bfloat16)
    own = jnp.concatenate([tokens, coef], axis=1)

    weights = []
    for count in range(nodes):
        held = (gate_weight[0, 0], up_weight[0, 0], down_weight[0, 0])
        weights += [send(w, node_shift(nodes, count)) for w in held] if count else held
    ids = jnp.stack([first_expert + (node - count) % nodes for count in range(nodes)])

    groups = grouping(layers)
    moved = {count: send(own, layer_shift(layers, count)) for count in range(1, layers)}
    moved[0] = own
    result = None
    for group in groups:
        unit = jnp.concatenate([moved[count] for count in group], axis=0)
        near = jnp.concatenate([unit, send(unit, first_partner)], axis=0)
        far = send(near, second_partner)
        kept, sent = run_experts(ids, near, far, weights)
        out = kept + send(sent, second_partner)
        half = out.shape[0] // 2
        out = out[:half] + send(out[half:].astype(jnp.bfloat16), first_partner)
        for at, count in enumerate(group):
            part = out[at * row_count : (at + 1) * row_count]
            if count:
                part = send(part.astype(jnp.bfloat16), layer_shift(layers, -count)).astype(jnp.float32)
            result = part if result is None else result + part
    return result.astype(jnp.bfloat16)


def solution(mesh):
    rows = P(("groups", "rail", "node"), None)
    weights = P("rail", "node", None, None)
    return jax.shard_map(
        layer,
        mesh=mesh,
        in_specs=(rows, rows, rows, weights, weights, weights),
        out_specs=rows,
        check_vma=False,
    )
```

```python
import functools

import jax
import jax.numpy as jnp
from jax import lax
from jax.experimental import pallas as pl
from jax.experimental.pallas import tpu as pltpu
from jax.sharding import PartitionSpec as P


SLICES = 8
LANES = 128
PLANE = 4
CHUNK = 1024


def send(block, target):
    rails, nodes = lax.axis_size("rail"), lax.axis_size("node")
    route = []
    for rail in range(rails):
        for node in range(nodes):
            rail_to, node_to = target(rail, node)
            route.append((rail * nodes + node, rail_to * nodes + node_to))
    return lax.ppermute(block, ("rail", "node"), route)


def first_partner(rail, node):
    return rail ^ (1 if node % 2 == 0 else 2), node


def second_partner(rail, node):
    return rail ^ (2 if node % 2 == 0 else 1), node


def layer_shift(layers, count):
    def target(rail, node):
        return (rail // PLANE + count) % layers * PLANE + rail % PLANE, node

    return target


def node_shift(nodes, count):
    return lambda rail, node: (rail, (node + count) % nodes)


def pieces(width):
    return [(start, min(CHUNK, width - start)) for start in range(0, width, CHUNK)]


def pack_kernel(tokens, routes, route_weight, packed):
    width = tokens.shape[1]
    lane = lax.broadcasted_iota(jnp.int32, (tokens.shape[0], LANES), 1)
    share = route_weight[...].astype(jnp.float32) / 256.0
    coef = jnp.zeros(lane.shape, jnp.float32)
    for at in range(routes.shape[1]):
        coef += jnp.where(lane == routes[:, at : at + 1], share[:, at : at + 1], 0.0)
    packed[:, :width] = tokens[...]
    packed[:, width:] = coef.astype(jnp.bfloat16)


def pack(tokens, routes, route_weight):
    rows, width = tokens.shape
    whole = pl.BlockSpec(memory_space=pltpu.VMEM)
    return pl.pallas_call(
        pack_kernel,
        in_specs=[whole] * 3,
        out_specs=whole,
        out_shape=jax.ShapeDtypeStruct((rows, width + LANES), jnp.bfloat16),
        compiler_params=pltpu.CompilerParams(vmem_limit_bytes=2 << 20),
    )(tokens, routes, route_weight)


def experts_kernel(ids, *refs, units, held):
    blocks, weights, outs = refs[: 2 * units], refs[2 * units : -2 * units], refs[-2 * units :]
    width = weights[0].shape[0]
    count = blocks[0].shape[0]
    lane = lax.broadcasted_iota(jnp.int32, (1, LANES), 1)
    coefs = jnp.concatenate([block[:, width:] for block in blocks], axis=0).astype(jnp.float32)
    hidden = []
    for at in range(held):
        w_gate, w_up, _ = weights[3 * at : 3 * at + 3]
        gate_vals = up_vals = None
        for start, size in pieces(width):
            rows = jnp.concatenate([block[:, start : start + size] for block in blocks], axis=0)
            gate_part = jnp.dot(rows, w_gate[start : start + size, :], preferred_element_type=jnp.float32)
            up_part = jnp.dot(rows, w_up[start : start + size, :], preferred_element_type=jnp.float32)
            gate_vals = gate_part if gate_vals is None else gate_vals + gate_part
            up_vals = up_part if up_vals is None else up_vals + up_part
        mine = jnp.sum(jnp.where(lane == ids[at], coefs, 0.0), axis=1, keepdims=True)
        silu = gate_vals / (1.0 + jnp.exp(-gate_vals))
        hidden.append((silu * up_vals * mine).astype(jnp.bfloat16))
    for start, size in pieces(width):
        total = None
        for at, value in enumerate(hidden):
            w_down = weights[3 * at + 2]
            part = jnp.dot(value, w_down[:, start : start + size], preferred_element_type=jnp.float32)
            total = part if total is None else total + part
        for at, out in enumerate(outs):
            out[:, start : start + size] = total[at * count : (at + 1) * count].astype(out.dtype)


def stage_kernel(*refs):
    held = (len(refs) - 1) // 2
    copies = [pltpu.make_async_copy(refs[at], refs[held + at], refs[2 * held].at[at]) for at in range(held)]
    for copy in copies:
        copy.start()
    for copy in copies:
        copy.wait()


def stage(weights):
    return pl.pallas_call(
        stage_kernel,
        in_specs=[pl.BlockSpec(memory_space=pltpu.HBM)] * len(weights),
        out_specs=tuple(pl.BlockSpec(memory_space=pltpu.VMEM) for _ in weights),
        out_shape=tuple(pltpu.VMEM(w.shape, w.dtype) for w in weights),
        scratch_shapes=[pltpu.SemaphoreType.DMA((len(weights),))],
        compiler_params=pltpu.CompilerParams(vmem_limit_bytes=1 << 20),
    )(*[pltpu.with_memory_space_constraint(w, pltpu.HBM) for w in weights])


def run_experts(ids, blocks, weights):
    width = weights[0].shape[0]
    rows = blocks[0].shape[0]
    flops = 2 * rows * len(blocks) * sum(w.size for w in weights)
    whole = pl.BlockSpec(memory_space=pltpu.VMEM)
    return pl.pallas_call(
        functools.partial(experts_kernel, units=len(blocks) // 2, held=len(weights) // 3),
        in_specs=[pl.BlockSpec(memory_space=pltpu.SMEM)] + [whole] * (len(blocks) + len(weights)),
        out_specs=(whole,) * len(blocks),
        out_shape=tuple(
            jax.ShapeDtypeStruct((rows, width), jnp.bfloat16 if at % 2 else jnp.float32) for at in range(len(blocks))
        ),
        cost_estimate=pl.CostEstimate(flops=flops, bytes_accessed=0, transcendentals=0),
        compiler_params=pltpu.CompilerParams(vmem_limit_bytes=8 << 20),
    )(ids, *blocks, *weights)


def shifts_of(layers):
    return sorted(range(1, layers), key=lambda count: min(count, layers - count))


def layer(tokens, routes, route_weight, gate_weight, up_weight, down_weight):
    row_count, _ = tokens.shape
    nodes = lax.axis_size("node")
    layers = lax.axis_size("rail") // PLANE
    node = lax.axis_index("node")
    first_expert = lax.axis_index("rail") // SLICES * nodes

    own = pack(tokens, routes, route_weight)

    weights = []
    for count in range(nodes):
        held = (gate_weight[0, 0], up_weight[0, 0], down_weight[0, 0])
        weights += [send(w, node_shift(nodes, count)) for w in held] if count else held
        weights[3 * count :] = stage(weights[3 * count :])
    ids = jnp.stack([first_expert + (node - count) % nodes for count in range(nodes)])

    shifts = shifts_of(layers)
    moved, blocks = {0: own}, {}
    for count in shifts:
        step = 1 if count <= layers // 2 else -1
        moved[count] = send(moved[(count - step) % layers], layer_shift(layers, step))
    for count, unit in moved.items():
        beside = send(unit, first_partner)
        near = jnp.concatenate([unit, beside], axis=0)
        blocks[count] = (near, send(near, second_partner))
    sums = {}
    for count in shifts:
        together = [count, 0] if count == shifts[0] else [count]
        outs = run_experts(ids, [block for unit in together for block in blocks[unit]], weights)
        for at, unit in enumerate(together):
            sums[unit] = outs[2 * at : 2 * at + 2]
    result = None
    for count in shifts + [0]:
        kept, sent = sums[count]
        back = send(sent, second_partner)
        out = kept + back
        back = send(out[row_count:].astype(jnp.bfloat16), first_partner)
        out = out[:row_count] + back
        if count:
            out = send(out.astype(jnp.bfloat16), layer_shift(layers, -count)).astype(jnp.float32)
        result = out if result is None else result + out
    return result.astype(jnp.bfloat16)


def solution(mesh):
    rows = P(("groups", "rail", "node"), None)
    weights = P("rail", "node", None, None)
    return jax.shard_map(
        layer,
        mesh=mesh,
        in_specs=(rows, rows, rows, weights, weights, weights),
        out_specs=rows,
        check_vma=False,
    )
```

```python
import functools

import jax
import jax.numpy as jnp
from jax import lax
from jax.experimental import pallas as pl
from jax.experimental.pallas import tpu as pltpu
from jax.sharding import PartitionSpec as P


SLICES = 8
LANES = 128
PLANE = 4
CHUNK = 1024


def send(block, target):
    rails, nodes = lax.axis_size("rail"), lax.axis_size("node")
    route = []
    for rail in range(rails):
        for node in range(nodes):
            rail_to, node_to = target(rail, node)
            route.append((rail * nodes + node, rail_to * nodes + node_to))
    return lax.ppermute(block, ("rail", "node"), route)


def first_partner(rail, node):
    return rail ^ (1 if node % 2 == 0 else 2), node


def second_partner(rail, node):
    return rail ^ (2 if node % 2 == 0 else 1), node


def layer_shift(layers, count):
    def target(rail, node):
        return (rail // PLANE + count) % layers * PLANE + rail % PLANE, node

    return target


def node_shift(nodes, count):
    return lambda rail, node: (rail, (node + count) % nodes)


def pieces(width):
    return [(start, min(CHUNK, width - start)) for start in range(0, width, CHUNK)]


def pack_kernel(tokens, routes, route_weight, packed, named, shares, arrived):
    width = tokens.shape[1]
    copies = [
        pltpu.make_async_copy(routes, named, arrived.at[0]),
        pltpu.make_async_copy(route_weight, shares, arrived.at[1]),
        pltpu.make_async_copy(tokens, packed.at[:, pl.ds(0, width)], arrived.at[2]),
    ]
    for copy in copies:
        copy.start()
    copies[0].wait()
    copies[1].wait()
    expert = lax.broadcasted_iota(jnp.int32, (LANES, tokens.shape[0]), 0)
    share = shares[...].astype(jnp.float32) / 256.0
    coef = jnp.zeros(expert.shape, jnp.float32)
    for at in range(routes.shape[0]):
        coef += jnp.where(expert == named[at : at + 1, :], share[at : at + 1, :], 0.0)
    packed[:, width:] = coef.T.astype(jnp.bfloat16)
    copies[2].wait()


def pack(tokens, routes, route_weight):
    rows, width = tokens.shape
    arrays = [pltpu.with_memory_space_constraint(a, pltpu.HBM) for a in (tokens, routes.T, route_weight.T)]
    return pl.pallas_call(
        pack_kernel,
        in_specs=[pl.BlockSpec(memory_space=pltpu.HBM)] * 3,
        out_specs=pl.BlockSpec(memory_space=pltpu.VMEM),
        out_shape=pltpu.VMEM((rows, width + LANES), jnp.bfloat16),
        scratch_shapes=[pltpu.VMEM(a.shape, a.dtype) for a in arrays[1:]] + [pltpu.SemaphoreType.DMA((3,))],
        compiler_params=pltpu.CompilerParams(vmem_limit_bytes=2 << 20),
    )(*arrays)


def experts_kernel(ids, *refs, units, held):
    blocks, weights, outs = refs[: 2 * units], refs[2 * units : -2 * units], refs[-2 * units :]
    width = weights[0].shape[0]
    count = blocks[0].shape[0]
    lane = lax.broadcasted_iota(jnp.int32, (1, LANES), 1)
    repeat = max(1, LANES // (2 * units * count))
    coefs = jnp.concatenate([block[:, width:] for block in blocks] * repeat, axis=0).astype(jnp.float32)
    hidden = []
    for at in range(held):
        w_gate, w_up, _ = weights[3 * at : 3 * at + 3]
        gate_vals = up_vals = None
        for start, size in pieces(width):
            rows = jnp.concatenate([block[:, start : start + size] for block in blocks] * repeat, axis=0)
            gate_part = jnp.dot(rows, w_gate[start : start + size, :], preferred_element_type=jnp.float32)
            up_part = jnp.dot(rows, w_up[start : start + size, :], preferred_element_type=jnp.float32)
            gate_vals = gate_part if gate_vals is None else gate_vals + gate_part
            up_vals = up_part if up_vals is None else up_vals + up_part
        mine = jnp.sum(jnp.where(lane == ids[at], coefs, 0.0), axis=1, keepdims=True)
        silu = gate_vals / (1.0 + jnp.exp(-gate_vals))
        hidden.append((silu * up_vals * mine).astype(jnp.bfloat16))
    for start, size in pieces(width):
        total = None
        for at, value in enumerate(hidden):
            w_down = weights[3 * at + 2]
            part = jnp.dot(value, w_down[:, start : start + size], preferred_element_type=jnp.float32)
            total = part if total is None else total + part
        for at, out in enumerate(outs):
            out[:, start : start + size] = total[at * count : (at + 1) * count].astype(out.dtype)


def stage_kernel(*refs):
    held = (len(refs) - 1) // 2
    copies = [pltpu.make_async_copy(refs[at], refs[held + at], refs[2 * held].at[at]) for at in range(held)]
    for copy in copies:
        copy.start()
    for copy in copies:
        copy.wait()


def stage(weights):
    return pl.pallas_call(
        stage_kernel,
        in_specs=[pl.BlockSpec(memory_space=pltpu.HBM)] * len(weights),
        out_specs=tuple(pl.BlockSpec(memory_space=pltpu.VMEM) for _ in weights),
        out_shape=tuple(pltpu.VMEM(w.shape, w.dtype) for w in weights),
        scratch_shapes=[pltpu.SemaphoreType.DMA((len(weights),))],
        compiler_params=pltpu.CompilerParams(vmem_limit_bytes=1 << 20),
    )(*[pltpu.with_memory_space_constraint(w, pltpu.HBM) for w in weights])


def run_experts(ids, blocks, weights):
    width = weights[0].shape[0]
    rows = blocks[0].shape[0]
    flops = 2 * rows * len(blocks) * sum(w.size for w in weights)
    whole = pl.BlockSpec(memory_space=pltpu.VMEM)
    return pl.pallas_call(
        functools.partial(experts_kernel, units=len(blocks) // 2, held=len(weights) // 3),
        in_specs=[pl.BlockSpec(memory_space=pltpu.SMEM)] + [whole] * (len(blocks) + len(weights)),
        out_specs=(whole,) * len(blocks),
        out_shape=tuple(
            jax.ShapeDtypeStruct((rows, width), jnp.bfloat16 if at % 2 else jnp.float32) for at in range(len(blocks))
        ),
        cost_estimate=pl.CostEstimate(flops=flops, bytes_accessed=0, transcendentals=0),
        compiler_params=pltpu.CompilerParams(vmem_limit_bytes=8 << 20),
    )(ids, *blocks, *weights)


def shifts_of(layers):
    return sorted(range(1, layers), key=lambda count: min(count, layers - count))


def calls_of(layers):
    shifts = shifts_of(layers)
    return [[shifts[0], 0]] + [shifts[at : at + 2][::-1] for at in range(1, len(shifts), 2)]


def layer(tokens, routes, route_weight, gate_weight, up_weight, down_weight):
    row_count, _ = tokens.shape
    nodes = lax.axis_size("node")
    layers = lax.axis_size("rail") // PLANE
    node = lax.axis_index("node")
    first_expert = lax.axis_index("rail") // SLICES * nodes

    own = pack(tokens, routes, route_weight)

    weights = []
    for count in range(nodes):
        held = (gate_weight[0, 0], up_weight[0, 0], down_weight[0, 0])
        weights += [send(w, node_shift(nodes, count)) for w in held] if count else held
        weights[3 * count :] = stage(weights[3 * count :])
    ids = jnp.stack([first_expert + (node - count) % nodes for count in range(nodes)])

    shifts = shifts_of(layers)
    moved, blocks = {0: own}, {}
    for count in shifts:
        step = 1 if count <= layers // 2 else -1
        moved[count] = send(moved[(count - step) % layers], layer_shift(layers, step))
    for count, unit in moved.items():
        beside = send(unit, first_partner)
        near = jnp.concatenate([unit, beside], axis=0)
        blocks[count] = (near, send(near, second_partner))
    sums = {}
    for together in calls_of(layers):
        outs = run_experts(ids, [block for unit in together for block in blocks[unit]], weights)
        for at, unit in enumerate(together):
            sums[unit] = outs[2 * at : 2 * at + 2]
    result = None
    for count in [unit for call in calls_of(layers) for unit in call if unit] + [0]:
        kept, sent = sums[count]
        back = send(sent, second_partner)
        out = kept + back
        back = send(out[row_count:].astype(jnp.bfloat16), first_partner)
        out = out[:row_count] + back
        out = out.astype(jnp.bfloat16) if count else out
        if count:
            out = send(out, layer_shift(layers, -count)).astype(jnp.float32)
        result = out if result is None else result + out
    return result.astype(jnp.bfloat16)


def solution(mesh):
    rows = P(("groups", "rail", "node"), None)
    weights = P("rail", "node", None, None)
    return jax.shard_map(
        layer,
        mesh=mesh,
        in_specs=(rows, rows, rows, weights, weights, weights),
        out_specs=rows,
        check_vma=False,
    )
```

```python
import functools

import jax
import jax.numpy as jnp
from jax import lax
from jax.experimental import pallas as pl
from jax.experimental.pallas import tpu as pltpu
from jax.sharding import PartitionSpec as P


SLICES = 8
LANES = 128
PLANE = 4
CHUNK = 1024
SIDE_IN = False


def send(block, target):
    rails, nodes = lax.axis_size("rail"), lax.axis_size("node")
    route = []
    for rail in range(rails):
        for node in range(nodes):
            rail_to, node_to = target(rail, node)
            route.append((rail * nodes + node, rail_to * nodes + node_to))
    return lax.ppermute(block, ("rail", "node"), route)


def first_partner(rail, node):
    return rail ^ (1 if node % 2 == 0 else 2), node


def second_partner(rail, node):
    return rail ^ (2 if node % 2 == 0 else 1), node


def layer_shift(layers, count):
    def target(rail, node):
        return (rail // PLANE + count) % layers * PLANE + rail % PLANE, node

    return target


def node_shift(nodes, count):
    return lambda rail, node: (rail, (node + count) % nodes)


def pieces(first, end):
    return [(start, min(CHUNK, end - start)) for start in range(first, end, CHUNK)]


def side_of(width):
    return width // LANES // 7 * LANES


def pack_kernel(tokens, routes, route_weight, packed, named, shares, arrived):
    width = tokens.shape[1]
    main = width - side_of(width)
    side = pl.ds(main, width - main)
    copies = [
        pltpu.make_async_copy(routes, named, arrived.at[0]),
        pltpu.make_async_copy(route_weight, shares, arrived.at[1]),
        pltpu.make_async_copy(tokens.at[:, pl.ds(0, main)], packed.at[:, pl.ds(0, main)], arrived.at[2]),
        pltpu.make_async_copy(tokens.at[:, side], packed.at[:, pl.ds(main + LANES, width - main)], arrived.at[3]),
    ]
    for copy in copies:
        copy.start()
    copies[0].wait()
    copies[1].wait()
    expert = lax.broadcasted_iota(jnp.int32, (LANES, tokens.shape[0]), 0)
    share = shares[...].astype(jnp.float32) / 256.0
    coef = jnp.zeros(expert.shape, jnp.float32)
    for at in range(routes.shape[0]):
        coef += jnp.where(expert == named[at : at + 1, :], share[at : at + 1, :], 0.0)
    packed[:, main : main + LANES] = coef.T.astype(jnp.bfloat16)
    copies[2].wait()
    copies[3].wait()


def pack(tokens, routes, route_weight):
    rows, width = tokens.shape
    arrays = [pltpu.with_memory_space_constraint(a, pltpu.HBM) for a in (tokens, routes.T, route_weight.T)]
    return pl.pallas_call(
        pack_kernel,
        in_specs=[pl.BlockSpec(memory_space=pltpu.HBM)] * 3,
        out_specs=pl.BlockSpec(memory_space=pltpu.VMEM),
        out_shape=pltpu.VMEM((rows, width + LANES), jnp.bfloat16),
        scratch_shapes=[pltpu.VMEM(a.shape, a.dtype) for a in arrays[1:]] + [pltpu.SemaphoreType.DMA((4,))],
        compiler_params=pltpu.CompilerParams(vmem_limit_bytes=2 << 20),
    )(*arrays)


def experts_kernel(ids, *refs, units, held):
    parts = 3 if SIDE_IN else 2
    blocks, weights, outs = refs[: parts * units], refs[parts * units : -3 * units], refs[-3 * units :]
    width = weights[0].shape[0]
    main = width - side_of(width)
    count = blocks[0].shape[0]
    lane = lax.broadcasted_iota(jnp.int32, (1, LANES), 1)
    repeat = max(1, LANES // (2 * units * count))
    firsts = [blocks[parts * unit + at] for unit in range(units) for at in range(2)]
    sides = [blocks[parts * unit + 2] for unit in range(units)] if SIDE_IN else None

    def rows_of(start, size):
        if start < main:
            taken = [block[:, start : start + size] for block in firsts]
        elif SIDE_IN:
            taken = [block[:, start - main : start - main + size] for block in sides]
        else:
            taken = [block[:, start + LANES : start + LANES + size] for block in firsts]
        return jnp.concatenate(taken * repeat, axis=0)

    spans = pieces(0, main) + pieces(main, width)
    coefs = jnp.concatenate([block[:, main : main + LANES] for block in firsts] * repeat, axis=0).astype(jnp.float32)
    hidden = []
    for at in range(held):
        w_gate, w_up, _ = weights[3 * at : 3 * at + 3]
        gate_vals = up_vals = None
        for start, size in spans:
            rows = rows_of(start, size)
            gate_part = jnp.dot(rows, w_gate[start : start + size, :], preferred_element_type=jnp.float32)
            up_part = jnp.dot(rows, w_up[start : start + size, :], preferred_element_type=jnp.float32)
            gate_vals = gate_part if gate_vals is None else gate_vals + gate_part
            up_vals = up_part if up_vals is None else up_vals + up_part
        mine = jnp.sum(jnp.where(lane == ids[at], coefs, 0.0), axis=1, keepdims=True)
        silu = gate_vals / (1.0 + jnp.exp(-gate_vals))
        hidden.append((silu * up_vals * mine).astype(jnp.bfloat16))
    for start, size in spans:
        total = None
        for at, value in enumerate(hidden):
            w_down = weights[3 * at + 2]
            part = jnp.dot(value, w_down[:, start : start + size], preferred_element_type=jnp.float32)
            total = part if total is None else total + part
        for unit in range(units):
            kept, sent, side = outs[3 * unit : 3 * unit + 3]
            own = total[2 * count * unit : 2 * count * (unit + 1)]
            if start < main:
                kept[:, start : start + size] = own[:count]
                sent[:, start : start + size] = own[count:].astype(sent.dtype)
            else:
                side[:, start - main : start - main + size] = own.astype(side.dtype)


def stage_kernel(*refs):
    held = (len(refs) - 1) // 2
    copies = [pltpu.make_async_copy(refs[at], refs[held + at], refs[2 * held].at[at]) for at in range(held)]
    for copy in copies:
        copy.start()
    for copy in copies:
        copy.wait()


def stage(weights):
    return pl.pallas_call(
        stage_kernel,
        in_specs=[pl.BlockSpec(memory_space=pltpu.HBM)] * len(weights),
        out_specs=tuple(pl.BlockSpec(memory_space=pltpu.VMEM) for _ in weights),
        out_shape=tuple(pltpu.VMEM(w.shape, w.dtype) for w in weights),
        scratch_shapes=[pltpu.SemaphoreType.DMA((len(weights),))],
        compiler_params=pltpu.CompilerParams(vmem_limit_bytes=1 << 20),
    )(*[pltpu.with_memory_space_constraint(w, pltpu.HBM) for w in weights])


def run_experts(ids, units, blocks, weights):
    width = weights[0].shape[0]
    side = side_of(width)
    rows = blocks[0].shape[0]
    flops = 2 * 2 * rows * len(units) * sum(w.size for w in weights)
    whole = pl.BlockSpec(memory_space=pltpu.VMEM)
    shapes = []
    for unit in units:
        shapes += [
            jax.ShapeDtypeStruct((rows, width - side), jnp.float32),
            jax.ShapeDtypeStruct((rows, width - side), jnp.bfloat16),
            jax.ShapeDtypeStruct((2 * rows, side), jnp.bfloat16 if unit else jnp.float32),
        ]
    return pl.pallas_call(
        functools.partial(experts_kernel, units=len(units), held=len(weights) // 3),
        in_specs=[pl.BlockSpec(memory_space=pltpu.SMEM)] + [whole] * (len(blocks) + len(weights)),
        out_specs=(whole,) * len(shapes),
        out_shape=tuple(shapes),
        cost_estimate=pl.CostEstimate(flops=flops, bytes_accessed=0, transcendentals=0),
        compiler_params=pltpu.CompilerParams(vmem_limit_bytes=8 << 20),
    )(ids, *blocks, *weights)


def shifts_of(layers):
    return sorted(range(1, layers), key=lambda count: min(count, layers - count))


def calls_of(layers):
    shifts = shifts_of(layers)
    return [[shifts[0], 0]] + [shifts[at : at + 2][::-1] for at in range(1, len(shifts), 2)]


def layer(tokens, routes, route_weight, gate_weight, up_weight, down_weight):
    row_count, model_width = tokens.shape
    nodes = lax.axis_size("node")
    layers = lax.axis_size("rail") // PLANE
    node = lax.axis_index("node")
    first_expert = lax.axis_index("rail") // SLICES * nodes

    own = pack(tokens, routes, route_weight)

    weights = []
    for count in range(nodes):
        held = (gate_weight[0, 0], up_weight[0, 0], down_weight[0, 0])
        weights += [send(w, node_shift(nodes, count)) for w in held] if count else held
        if count:
            weights[3 * count :] = stage(weights[3 * count :])
    ids = jnp.stack([first_expert + (node - count) % nodes for count in range(nodes)])

    shifts = shifts_of(layers)
    side = side_of(model_width)
    main = model_width - side
    moved, blocks = {0: own}, {}
    steps = {count: 1 if count <= layers // 2 else -1 for count in shifts}
    for count in shifts:
        source = moved[(count - steps[count]) % layers]
        if SIDE_IN:
            source = source[:, : main + LANES]
        moved[count] = send(source, layer_shift(layers, steps[count]))
    for count, unit in moved.items():
        beside = send(unit, first_partner)
        near = jnp.concatenate([unit, beside], axis=0)
        blocks[count] = [near, send(near, second_partner)]
    if SIDE_IN:
        blocks[0].append(jnp.concatenate([block[:, main + LANES :] for block in blocks[0]], axis=0))
        for count in shifts:
            source = blocks[(count - steps[count]) % layers][2]
            blocks[count].append(send(source, layer_shift(layers, steps[count])))
    sums = {}
    for together in calls_of(layers):
        outs = run_experts(ids, together, [block for unit in together for block in blocks[unit]], weights)
        for at, unit in enumerate(together):
            sums[unit] = outs[3 * at : 3 * at + 3]
    backs = [unit for call in calls_of(layers) for unit in call if unit]
    arrived = [send(sums[count][2], layer_shift(layers, -count)) for count in backs]
    result = None
    for count in backs + [0]:
        kept, sent, own_side = sums[count]
        if not count:
            for piece in arrived:
                own_side = own_side + piece.astype(jnp.float32)
            kept = jnp.concatenate([kept, own_side[: kept.shape[0]]], axis=1)
            sent = jnp.concatenate([sent, own_side[kept.shape[0] :].astype(jnp.bfloat16)], axis=1)
            result = jnp.pad(result, ((0, 0), (0, side)))
        back = send(sent, second_partner)
        out = kept + back
        back = send(out[row_count:].astype(jnp.bfloat16), first_partner)
        out = out[:row_count] + back
        out = out.astype(jnp.bfloat16) if count else out
        if count:
            out = send(out, layer_shift(layers, -count)).astype(jnp.float32)
        result = out if result is None else result + out
    return result.astype(jnp.bfloat16)


def solution(mesh):
    rows = P(("groups", "rail", "node"), None)
    weights = P("rail", "node", None, None)
    return jax.shard_map(
        layer,
        mesh=mesh,
        in_specs=(rows, rows, rows, weights, weights, weights),
        out_specs=rows,
        check_vma=False,
    )
```
